32 devices in a mesh: task: 4 (over y, x), param: 8 (over z, core).
Axes of the slice: x: 2, y: 2, z: 4, core: 2. Of those that a mesh axis runs over, the one named last changes fastest.
Arguments:
- grads: bfloat16 [8, 2048, 4096], P('task', 'param')
- order: int32 [8], replicated, may hold values from 0 to 7, each once
Outputs:
- update: float32 [2048, 4096], P('param', 'task')
The draws below stay inside these ranges and needn't reach their ends.
All inputs are finite; a program needn't handle non-finite values.
Results may differ from the reference program's by a relative error of at most 0.0003.
Values may be sent and summed in bfloat16 or wider, within the bound.
A program may use at most 64 MiB of HBM per device.

```python
import jax
import jax.numpy as jnp
from jax import lax

FF = 4096
ROW_DEV = 256
TASKS = 8
ROWS = 2048


def draw_grads(key, part):
    keys = jax.random.split(jax.random.fold_in(key, 11), 5)
    blocks = ROWS // ROW_DEV
    cols = FF // 8
    base = jax.random.uniform(keys[0], (TASKS, blocks, 1, 8, 1), jnp.float32, -1.5, 1.5)
    row_part = jax.random.uniform(keys[4], (TASKS, blocks, ROW_DEV, 8, 1), jnp.float32, -2.0, 2.0)
    mixing = base + row_part
    shared = jax.random.normal(keys[1], (1, blocks, ROW_DEV, 8, cols), jnp.float32)
    noise = jax.random.normal(keys[2], (TASKS, blocks, ROW_DEV, 8, cols), jnp.float32)
    scales = jnp.exp(jax.random.uniform(keys[3], (1, blocks, 1, 8, 1), jnp.float32, 0.0, 2.3))
    values = (mixing * shared + noise) * scales
    return values.reshape(TASKS, ROWS, FF).astype(jnp.bfloat16)


def setup_inputs(seed: int = 0) -> dict:
    key_of = jax.random.split(jax.random.key(seed), 3)
    return {
        "grads": draw_grads(jax.random.fold_in(key_of[2], 71), 0),
        "order": jax.random.permutation(key_of[1], TASKS).astype(jnp.int32),
    }


def reference(grads, order):
    flat = grads.reshape(TASKS, -1)
    gram = lax.dot_general(flat, flat, (((1,), (1,)), ((), ())), preferred_element_type=jnp.float32)
    coefs = jnp.eye(TASKS, dtype=jnp.float32)
    labels = jnp.arange(TASKS, dtype=jnp.int32)
    for k in range(TASKS):
        j = order[k]
        picked = (labels == j).astype(jnp.float32)
        column = lax.optimization_barrier(jnp.sum(gram * picked[None, :], axis=1))
        d = lax.optimization_barrier(jnp.sum(coefs * column[None, :], axis=1))
        norm_j = jnp.sum(column * picked)
        w = jnp.minimum(d, 0.0) / (norm_j + 1e-06)
        w = w * (1.0 - picked)
        coefs = coefs - w[:, None] * picked[None, :]
    weight = lax.optimization_barrier(jnp.sum(coefs, axis=0))
    combined = jnp.zeros((ROWS, FF), jnp.float32)
    for m in range(TASKS):
        combined = combined + weight[m] * grads[m].astype(jnp.float32)
    rms = jnp.sqrt(jnp.sum(combined * combined) / (ROWS * FF) + 1e-06)
    return combined * (0.5 / rms)
```

```python
import functools

import jax
import jax.numpy as jnp
from jax import lax
from jax.experimental import pallas as pl
from jax.experimental.pallas import tpu as pltpu
from jax.sharding import PartitionSpec as P

MESH = pl.DeviceIdType.MESH
LANES = 128
TILE = 16
CHUNKS = 8


def kernel(
    n_task, n_param, entries,
    order_hbm, grads_ref, out_ref,
    order_ref, mine, gp, gt,
    order_sem, own_sem, send_sem, recv_sem, p_send, p_recv, t_send, t_recv,
):
    tasks_here, rows, _ = grads_ref.shape
    total, _, block = mine.shape
    lane_blocks = block // LANES
    chunk = rows // CHUNKS
    t = lax.axis_index("task")
    p = lax.axis_index("param")

    def to_t(d):
        if n_task == 4:
            return (t + 1 - 2 * lax.rem(t, 2), lax.rem(t + 2, 4), 3 - t)[d - 1]
        return lax.rem(t + d, n_task)

    def from_t(d):
        return to_t(d) if n_task == 4 else lax.rem(t - d + n_task, n_task)

    def peer_t(d):
        return {"task": to_t(d)}

    def peer_p(d):
        return {"param": lax.rem(p + d, n_param)}

    def cols(of):
        return pl.ds(pl.multiple_of(of * block, LANES), block)

    def rows_of(c):
        return pl.ds(pl.multiple_of(c * chunk, TILE), chunk)

    def exchange(d, c, slot):
        return pltpu.make_async_remote_copy(
            src_ref=grads_ref.at[:, rows_of(c), cols(to_t(d))],
            dst_ref=mine.at[pl.ds(slot * tasks_here, tasks_here), rows_of(c), :],
            send_sem=send_sem.at[d - 1, c],
            recv_sem=recv_sem.at[d - 1, c],
            device_id=peer_t(d),
            device_id_type=MESH,
        )

    def local(c):
        return pltpu.make_async_copy(
            grads_ref.at[:, rows_of(c), cols(t)],
            mine.at[pl.ds(t * tasks_here, tasks_here), rows_of(c), :],
            own_sem.at[c],
        )

    barrier = pltpu.get_barrier_semaphore()
    for d in range(1, n_task):
        pl.semaphore_signal(barrier, inc=1, device_id=peer_t(d), device_id_type=MESH)
    for d in range(1, n_param):
        pl.semaphore_signal(barrier, inc=1, device_id=peer_p(d), device_id_type=MESH)
    pl.semaphore_wait(barrier, n_task + n_param - 2)

    far = n_task - 1
    for c in range(CHUNKS):
        exchange(far, c, t).start()
    for c in range(CHUNKS):
        local(c).start()
    get_order = pltpu.make_async_copy(order_hbm, order_ref, order_sem)
    get_order.start()
    for c in range(CHUNKS):
        for d in range(1, far):
            exchange(d, c, t).start()

    pairs = [(i, j) for i in range(total) for j in range(i, total)]
    steps = chunk // TILE * lane_blocks

    def tile_of(q):
        r = pl.multiple_of(q // lane_blocks * TILE, TILE)
        l = pl.multiple_of(q % lane_blocks * LANES, LANES)
        return pl.ds(r, TILE), pl.ds(l, LANES)

    def gram_chunk(c, accs):
        local(c).wait()
        for d in range(1, n_task):
            exchange(d, c, from_t(d)).wait_recv()

        def step(q, accs):
            r, l = tile_of(q + c * steps)
            x = [mine[m, r, l].astype(jnp.float32) for m in range(total)]
            out = []
            for acc, (i, j) in zip(accs, pairs):
                prod = x[i] * x[j]
                out.append(acc + (prod[:8] + prod[8:]))
            return tuple(out)

        return lax.fori_loop(0, steps, step, accs)

    zero = jnp.zeros((8, LANES), jnp.float32)
    accs = lax.fori_loop(0, CHUNKS, gram_chunk, (zero,) * len(pairs))

    sub = lax.broadcasted_iota(jnp.int32, (8, LANES), 0)
    lane = lax.broadcasted_iota(jnp.int32, (8, LANES), 1)
    by_pair = dict(zip(pairs, accs))
    summed = {
        k: jnp.broadcast_to(jnp.sum(v, axis=0, keepdims=True), (8, LANES))
        for k, v in by_pair.items()
    }
    packed = zero
    for i in range(total):
        stacked = zero
        for j in range(total):
            stacked = jnp.where(sub == j, summed[min(i, j), max(i, j)], stacked)
        here = lane == sub * total + i
        packed = jnp.where(here, jnp.sum(stacked, axis=1, keepdims=True), packed)

    gp[p] = jnp.sum(packed, axis=0, keepdims=True)

    def send_p(d, slot):
        return pltpu.make_async_remote_copy(
            src_ref=gp.at[p], dst_ref=gp.at[slot],
            send_sem=p_send.at[d - 1], recv_sem=p_recv.at[d - 1],
            device_id=peer_p(d), device_id_type=MESH,
        )

    def send_t(d, slot):
        return pltpu.make_async_remote_copy(
            src_ref=gt.at[t], dst_ref=gt.at[slot],
            send_sem=t_send.at[d - 1], recv_sem=t_recv.at[d - 1],
            device_id=peer_t(d), device_id_type=MESH,
        )

    for d in range(1, n_param):
        send_p(d, p).start()
    for d in range(1, n_param):
        send_p(d, lax.rem(p - d + n_param, n_param)).wait_recv()
    part = gp[0]
    for k in range(1, n_param):
        part = part + gp[k]
    gt[t] = part
    for d in range(1, n_task):
        send_t(d, t).start()
    for d in range(1, n_task):
        send_t(d, from_t(d)).wait_recv()
    gram = gt[0]
    for k in range(1, n_task):
        gram = gram + gt[k]
    gram = jnp.broadcast_to(gram, (8, LANES))

    get_order.wait()
    coefs = jnp.where((sub == lane) & (sub < total), 1.0, 0.0)
    columns, norms = [], []
    for k in range(total):
        j = order_ref[k]
        column = jnp.sum(jnp.where(lane == sub * total + j, gram, 0.0), axis=1, keepdims=True)
        column = jnp.broadcast_to(column, (8, LANES))
        columns.append(column)
        norms.append(jnp.sum(jnp.where(sub == j, column, 0.0), axis=0, keepdims=True))
    for k in range(total):
        j = order_ref[k]
        d = jnp.sum(coefs * columns[k], axis=0, keepdims=True)
        w = jnp.minimum(d, 0.0) / (norms[k] + 1e-06)
        w = jnp.broadcast_to(w, (8, LANES))
        coefs = coefs - jnp.where((sub == j) & (lane != j), w, 0.0)
    weight = jnp.broadcast_to(jnp.sum(coefs, axis=1, keepdims=True), (8, LANES))
    spread = jnp.where(lax.rem(lane, total) == sub, weight, 0.0)
    across = jnp.sum(spread, axis=0, keepdims=True)
    row_m = (lane >= sub * total) & (lane < sub * total + total)
    half = jnp.sum(jnp.where(row_m, gram * across, 0.0), axis=1, keepdims=True)
    energy = jnp.sum(weight * half, axis=0, keepdims=True)
    rms = jnp.sqrt(jnp.maximum(energy, 0.0) / entries + 1e-06)
    scaled = weight * (0.5 / rms)
    each = [jnp.broadcast_to(scaled[m : m + 1, :], (TILE, LANES)) for m in range(total)]

    def combine(q, carry):
        r, l = tile_of(q)
        v = each[0] * mine[0, r, l].astype(jnp.float32)
        for m in range(1, total):
            v = v + each[m] * mine[m, r, l].astype(jnp.float32)
        out_ref[r, l] = v
        return carry

    lax.fori_loop(0, rows // TILE * lane_blocks, combine, 0, unroll=4)
    for c in range(CHUNKS):
        for d in range(1, n_task):
            exchange(d, c, t).wait_send()
    for d in range(1, n_param):
        send_p(d, p).wait_send()
    for d in range(1, n_task):
        send_t(d, t).wait_send()


def shards(mesh, grads, order):
    n_task, n_param = mesh.shape["task"], mesh.shape["param"]
    tasks_here, rows, width = grads.shape
    total, block = tasks_here * n_task, width // n_task
    entries = float(rows * n_param * width)
    dma = pltpu.SemaphoreType.DMA
    return pl.pallas_call(
        functools.partial(kernel, n_task, n_param, entries),
        out_shape=pltpu.VMEM((rows, block), jnp.float32),
        in_specs=[
            pl.BlockSpec(memory_space=pltpu.HBM),
            pl.BlockSpec(memory_space=pltpu.HBM),
        ],
        out_specs=pl.BlockSpec(memory_space=pltpu.VMEM),
        scratch_shapes=[
            pltpu.SMEM((total,), jnp.int32),
            pltpu.VMEM((total, rows, block), jnp.bfloat16),
            pltpu.VMEM((n_param, 1, LANES), jnp.float32),
            pltpu.VMEM((n_task, 1, LANES), jnp.float32),
            dma(()),
            dma((CHUNKS,)),
            dma((n_task - 1, CHUNKS)),
            dma((n_task - 1, CHUNKS)),
            dma((n_param - 1,)),
            dma((n_param - 1,)),
            dma((n_task - 1,)),
            dma((n_task - 1,)),
        ],
        compiler_params=pltpu.CompilerParams(collective_id=0, has_side_effects=True),
    )(order, grads)


def solution(mesh):
    placed = (P("task", "param", None), P())
    return jax.shard_map(
        functools.partial(shards, mesh),
        mesh=mesh, in_specs=placed, out_specs=P("param", "task"), check_vma=False,
    )
```

```python
import functools

import jax
import jax.numpy as jnp
from jax import lax
from jax.experimental import pallas as pl
from jax.experimental.pallas import tpu as pltpu
from jax.sharding import PartitionSpec as P

MESH = pl.DeviceIdType.MESH
LANES = 128
TILE = 16
CHUNKS = 8


def kernel(
    n_task, n_param, entries,
    order_hbm, grads_ref, out_ref,
    order_ref, mine, parts,
    order_sem, own_sem, send_sem, recv_sem, g_send, g_recv, known,
):
    tasks_here, rows, _ = grads_ref.shape
    total, _, block = mine.shape
    lane_blocks = block // LANES
    chunk = rows // CHUNKS
    t = lax.axis_index("task")
    p = lax.axis_index("param")

    def to_t(d):
        if n_task == 4:
            return (t + 1 - 2 * lax.rem(t, 2), lax.rem(t + 2, 4), 3 - t)[d - 1]
        return lax.rem(t + d, n_task)

    def from_t(d):
        return to_t(d) if n_task == 4 else lax.rem(t - d + n_task, n_task)

    def peer_t(d):
        return {"task": to_t(d)}

    pair = 2 if n_param % 2 == 0 else 1
    close = (1, 2) if n_task == 4 else tuple(range(1, n_task))
    up, down = p + pair < n_param, p >= pair
    degree = len(close) + pair - 1 + up.astype(jnp.int32) + down.astype(jnp.int32)

    def greet(sem):
        for d in close:
            pl.semaphore_signal(sem, inc=1, device_id=peer_t(d), device_id_type=MESH)
        if pair == 2:
            other = {"param": p + 1 - 2 * lax.rem(p, 2)}
            pl.semaphore_signal(sem, inc=1, device_id=other, device_id_type=MESH)

        @pl.when(up)
        def _():
            pl.semaphore_signal(sem, inc=1, device_id={"param": p + pair}, device_id_type=MESH)

        @pl.when(down)
        def _():
            pl.semaphore_signal(sem, inc=1, device_id={"param": p - pair}, device_id_type=MESH)

        pl.semaphore_wait(sem, degree)

    def cols(of):
        return pl.ds(pl.multiple_of(of * block, LANES), block)

    def rows_of(c):
        return pl.ds(pl.multiple_of(c * chunk, TILE), chunk)

    def exchange(d, c, slot):
        return pltpu.make_async_remote_copy(
            src_ref=grads_ref.at[:, rows_of(c), cols(to_t(d))],
            dst_ref=mine.at[pl.ds(slot * tasks_here, tasks_here), rows_of(c), :],
            send_sem=send_sem.at[d - 1, c],
            recv_sem=recv_sem.at[d - 1, c],
            device_id=peer_t(d),
            device_id_type=MESH,
        )

    def local(c):
        return pltpu.make_async_copy(
            grads_ref.at[:, rows_of(c), cols(t)],
            mine.at[pl.ds(t * tasks_here, tasks_here), rows_of(c), :],
            own_sem.at[c],
        )

    greet(pltpu.get_barrier_semaphore())
    rounds = spread_rounds(n_task, n_param)
    for d in close:
        exchange(d, 0, t).start()
    for k in range(min(1, rounds)):
        greet(known.at[k])
    for d in range(1, n_task):
        if d not in close:
            for c in range(CHUNKS):
                exchange(d, c, t).start()
    for c in range(1, CHUNKS):
        for d in close:
            exchange(d, c, t).start()
    for c in range(CHUNKS):
        local(c).start()
    get_order = pltpu.make_async_copy(order_hbm, order_ref, order_sem)
    get_order.start()
    for k in range(1, rounds):
        greet(known.at[k])
    get_order.wait()

    pairs = [(i, j) for i in range(total) for j in range(i, total)]
    steps = chunk // TILE * lane_blocks

    def tile_of(q):
        r = pl.multiple_of(q // lane_blocks * TILE, TILE)
        l = pl.multiple_of(q % lane_blocks * LANES, LANES)
        return pl.ds(r, TILE), pl.ds(l, LANES)

    def gram_chunk(c, accs):
        local(c).wait()
        for d in range(1, n_task):
            exchange(d, c, from_t(d)).wait_recv()

        def step(q, accs):
            r, l = tile_of(q + c * steps)
            x = [mine[m, r, l].astype(jnp.float32) for m in range(total)]
            out = []
            for acc, (i, j) in zip(accs, pairs):
                prod = x[i] * x[j]
                out.append(acc + (prod[:8] + prod[8:]))
            return tuple(out)

        return lax.fori_loop(0, steps, step, accs)

    zero = jnp.zeros((8, LANES), jnp.float32)
    accs = lax.fori_loop(0, CHUNKS, gram_chunk, (zero,) * len(pairs))

    sub = lax.broadcasted_iota(jnp.int32, (8, LANES), 0)
    lane = lax.broadcasted_iota(jnp.int32, (8, LANES), 1)
    by_pair = dict(zip(pairs, accs))
    summed = {
        k: jnp.broadcast_to(jnp.sum(v, axis=0, keepdims=True), (8, LANES))
        for k, v in by_pair.items()
    }
    packed = zero
    for i in range(total):
        stacked = zero
        for j in range(total):
            stacked = jnp.where(sub == j, summed[min(i, j), max(i, j)], stacked)
        here = lane == sub * total + i
        packed = jnp.where(here, jnp.sum(stacked, axis=1, keepdims=True), packed)

    me = p * n_task + t
    everyone = [(dp, dt) for dp in range(n_param) for dt in range(n_task) if dp or dt]
    everyone.sort(key=lambda k: abs(k[0] - n_param // 2))
    parts[me] = jnp.sum(packed, axis=0, keepdims=True)

    def share(k):
        dp, dt = everyone[k]
        return pltpu.make_async_remote_copy(
            src_ref=parts.at[me], dst_ref=parts.at[me],
            send_sem=g_send, recv_sem=g_recv,
            device_id={"param": lax.rem(p + dp, n_param), "task": lax.rem(t + dt, n_task)},
            device_id_type=MESH,
        )

    def shared(sem):
        count = pl.ds(0, len(everyone))
        return pltpu.make_async_copy(parts.at[count], parts.at[count], sem)

    for k in range(len(everyone)):
        share(k).start()
    for c in range(CHUNKS):
        for d in range(1, n_task):
            exchange(d, c, t).wait_send()
    shared(g_recv).wait()
    terms = [parts[k] for k in range(n_task * n_param)]
    while len(terms) > 1:
        odd = terms[len(terms) - len(terms) % 2 :]
        terms = [a + b for a, b in zip(terms[0::2], terms[1::2])] + odd
    gram = jnp.broadcast_to(terms[0], (8, LANES))

    coefs = jnp.where((sub == lane) & (sub < total), 1.0, 0.0)
    columns, norms = [], []
    for k in range(total):
        j = order_ref[k]
        column = jnp.sum(jnp.where(lane == sub * total + j, gram, 0.0), axis=1, keepdims=True)
        column = jnp.broadcast_to(column, (8, LANES))
        columns.append(column)
        norms.append(jnp.sum(jnp.where(sub == j, column, 0.0), axis=0, keepdims=True))
    for k in range(total):
        j = order_ref[k]
        d = jnp.sum(coefs * columns[k], axis=0, keepdims=True)
        w = jnp.minimum(d, 0.0) / (norms[k] + 1e-06)
        w = jnp.broadcast_to(w, (8, LANES))
        coefs = coefs - jnp.where((sub == j) & (lane != j), w, 0.0)
    weight = jnp.broadcast_to(jnp.sum(coefs, axis=1, keepdims=True), (8, LANES))
    spread = jnp.where(lax.rem(lane, total) == sub, weight, 0.0)
    across = jnp.sum(spread, axis=0, keepdims=True)
    row_m = (lane >= sub * total) & (lane < sub * total + total)
    half = jnp.sum(jnp.where(row_m, gram * across, 0.0), axis=1, keepdims=True)
    energy = jnp.sum(weight * half, axis=0, keepdims=True)
    rms = jnp.sqrt(jnp.maximum(energy, 0.0) / entries + 1e-06)
    scaled = weight * (0.5 / rms)
    each = [jnp.broadcast_to(scaled[m : m + 1, :], (TILE, LANES)) for m in range(total)]

    def combine(q, carry):
        r, l = tile_of(q)
        v = each[0] * mine[0, r, l].astype(jnp.float32)
        for m in range(1, total):
            v = v + each[m] * mine[m, r, l].astype(jnp.float32)
        out_ref[r, l] = v
        return carry

    lax.fori_loop(0, rows // TILE * lane_blocks, combine, 0, unroll=4)
    shared(g_send).wait()


def spread_rounds(n_task, n_param):
    pair = 2 if n_param % 2 == 0 else 1
    return (2 if n_task == 4 else 1) + pair - 1 + n_param // pair - 1 - 1


def shards(mesh, grads, order):
    n_task, n_param = mesh.shape["task"], mesh.shape["param"]
    tasks_here, rows, width = grads.shape
    total, block = tasks_here * n_task, width // n_task
    entries = float(rows * n_param * width)
    dma = pltpu.SemaphoreType.DMA
    return pl.pallas_call(
        functools.partial(kernel, n_task, n_param, entries),
        out_shape=pltpu.VMEM((rows, block), jnp.float32),
        in_specs=[
            pl.BlockSpec(memory_space=pltpu.HBM),
            pl.BlockSpec(memory_space=pltpu.HBM),
        ],
        out_specs=pl.BlockSpec(memory_space=pltpu.VMEM),
        scratch_shapes=[
            pltpu.SMEM((total,), jnp.int32),
            pltpu.VMEM((total, rows, block), jnp.bfloat16),
            pltpu.VMEM((n_task * n_param, 1, LANES), jnp.float32),
            dma(()),
            dma((CHUNKS,)),
            dma((n_task - 1, CHUNKS)),
            dma((n_task - 1, CHUNKS)),
            dma(()),
            dma(()),
            pltpu.SemaphoreType.REGULAR((max(1, spread_rounds(n_task, n_param)),)),
        ],
        compiler_params=pltpu.CompilerParams(collective_id=0, has_side_effects=True),
    )(order, grads)


def solution(mesh):
    placed = (P("task", "param", None), P())
    return jax.shard_map(
        functools.partial(shards, mesh),
        mesh=mesh, in_specs=placed, out_specs=P("param", "task"), check_vma=False,
    )
```
